512 devices in a mesh: ctx: 64 (over x, z_lo, core), head: 8 (over y, z_hi).
Axes of the slice: x: 4, y: 4, z: 16 (z_hi: 2, z_lo: 8; z = z_hi * 8 + z_lo), core: 2. Of those that a mesh axis runs over, the one named last changes fastest.
Arguments:
- query_heads: bfloat16 [8192, 64, 576], P('ctx', 'head'), may hold values from -16 to 16
- key_latent: bfloat16 [8192, 576], P('ctx'), may hold values from -6 to 6
- doc_start: int32 [8192], P('ctx'), may hold values from 0 to 8191, as said below
- out_grad: bfloat16 [8192, 64, 512], P('ctx', 'head'), may hold values from -12 to 12
Outputs:
- attention: bfloat16 [8192, 64, 512], P('ctx', 'head')
- d_query: bfloat16 [8192, 64, 576], P('ctx', 'head')
- d_key: float32 [8192, 576], P(('ctx', 'head'))
The draws below stay inside these ranges and needn't reach their ends.
Inputs may be any that keep to these rules, and one draw needn't show every extreme that they name: doc_start[t] <= t; doc_start[t] is t or doc_start[t - 1]; every document holds at most 256 tokens, and some document holds exactly 256.
All inputs are finite; a program needn't handle non-finite values.
Results may differ from the reference program's by a relative error of at most 0.013.
Values may be sent and summed in bfloat16 or wider, within the bound.
No kernel may reach another device: no remote copies, remote signals or barrier semaphores. Data moves between devices by JAX's collectives and lax.ppermute only.
A program may use at most 64 MiB of HBM per device.

```python
import jax
import jax.numpy as jnp
from jax import lax

HEADS = 64
LAT = 512
MAXDOC = 256
TOK_DEV = 128
DQK = 576
TOKENS = 8192


def common_draw(key):
    positions = jnp.arange(TOKENS, dtype=jnp.int32)
    choose = jax.random.randint(jax.random.fold_in(key, 11), (TOKENS,), 0, 2)
    longer = jax.random.randint(jax.random.fold_in(key, 12), (TOKENS,), MAXDOC // 2, MAXDOC + 1)
    shorter = jax.random.randint(jax.random.fold_in(key, 13), (TOKENS,), 1, MAXDOC // 8 + 1)
    forced = jax.random.randint(jax.random.fold_in(key, 14), (), 0, 4)
    lengths = jnp.where(choose == 0, longer, shorter)
    lengths = jnp.where(positions == forced, MAXDOC, lengths).astype(jnp.int32)
    endings = jnp.cumsum(lengths).astype(jnp.int32)
    beginnings = endings - lengths
    doc_index = jnp.searchsorted(endings, positions, side='right').astype(jnp.int32)
    doc_first = beginnings[doc_index].astype(jnp.int32)
    key_rows = jnp.clip(jax.random.normal(jax.random.fold_in(key, 21), (TOKENS, DQK), jnp.float32), -6.0, 6.0)
    queries = jnp.clip(jax.random.normal(jax.random.fold_in(key, 23), (TOKENS, HEADS, DQK), jnp.float32), -6.0, 6.0)
    return (doc_first, queries, key_rows)


def draw_query_heads(key, part):
    return common_draw(key)[1].astype(jnp.bfloat16)


def draw_key_latent(key, part):
    return common_draw(key)[2].astype(jnp.bfloat16)


def draw_doc_start(key, part):
    return common_draw(key)[0].astype(jnp.int32)


def level_of(own_key, dims, pieces, least, high):
    def one(position, parts):
        heights = jax.random.uniform(jax.random.fold_in(jax.random.fold_in(own_key, 6), position), (parts,), jnp.float32, least / len(pieces), high / len(pieces))
        return jnp.repeat(jnp.exp(heights), dims[position] // parts).reshape((-1,) + (1,) * (len(dims) - position - 1))

    loudness = one(*pieces[0])
    for cut in pieces[1:]:
        loudness = loudness * one(*cut)
    return loudness


def gaussian(rng, shape, spread, limit, cuts=(), held_as=jnp.bfloat16):
    loudness = level_of(rng, shape, cuts, -0.22, 0.18) if cuts else 1.0
    entries = jax.random.normal(rng, shape, jnp.float32) * spread * loudness
    return jnp.minimum(jnp.maximum(entries, -limit), limit).astype(held_as)


def setup_inputs(seed: int = 0) -> dict:
    keys = jax.random.split(jax.random.key(seed), 5)
    query_heads = draw_query_heads(jax.random.fold_in(keys[4], 71), 0)
    key_latent = draw_key_latent(jax.random.fold_in(keys[4], 71), 0)
    doc_start = draw_doc_start(jax.random.fold_in(keys[4], 71), 0)
    out_grad = gaussian(keys[3], (TOKENS, HEADS, LAT), 2.0, 12.0, ((0, 64), (1, 8)))
    return dict(query_heads=query_heads, key_latent=key_latent, doc_start=doc_start, out_grad=out_grad)


score_scale = 192 ** -0.5


def reference(query_heads, key_latent, doc_start, out_grad):
    reach = (MAXDOC + TOK_DEV - 2) // TOK_DEV
    span = (reach + 1) * TOK_DEV
    block_count = TOKENS // TOK_DEV
    padded = jnp.concatenate([jnp.zeros((reach * TOK_DEV, DQK), jnp.bfloat16), key_latent], axis=0)

    def one_block(carried, block_index):
        start = (block_index * TOK_DEV).astype(jnp.int32)
        window = lax.dynamic_slice_in_dim(padded, start, span, 0).astype(jnp.float32)
        queries = lax.dynamic_slice_in_dim(query_heads, start, TOK_DEV, 0).astype(jnp.float32)
        cotangent = lax.dynamic_slice_in_dim(out_grad, start, TOK_DEV, 0).astype(jnp.float32)
        doc_first = lax.dynamic_slice_in_dim(doc_start, start, TOK_DEV, 0)
        query_pos = start + jnp.arange(TOK_DEV, dtype=jnp.int32)
        key_pos = start - reach * TOK_DEV + jnp.arange(span, dtype=jnp.int32)
        visible = (key_pos[None, :] >= doc_first[:, None]) & (key_pos[None, :] <= query_pos[:, None])
        scores = jnp.einsum("thd,kd->thk", queries, window) * score_scale
        scores = jnp.where(visible[:, None, :], scores, -jnp.inf)
        top = jnp.max(scores, axis=2, keepdims=True)
        expon = jnp.exp(scores - top)
        probs = expon / jnp.sum(expon, axis=2, keepdims=True)
        weights = probs.astype(jnp.bfloat16).astype(jnp.float32)
        values = window[:, :LAT]
        attention = jnp.einsum("thk,kc->thc", weights, values).astype(jnp.bfloat16)
        dprob = jnp.einsum("thc,kc->thk", cotangent, values)
        row_delta = jnp.sum(probs * dprob, axis=2, keepdims=True)
        dscore = (score_scale * probs * (dprob - row_delta)).astype(jnp.bfloat16).astype(jnp.float32)
        d_query = jnp.einsum("thk,kd->thd", dscore, window).astype(jnp.bfloat16)
        from_scores = jnp.einsum("thk,thd->kd", dscore, queries)
        from_values = jnp.einsum("thk,thc->kc", weights, cotangent)
        window_grad = from_scores + jnp.pad(from_values, ((0, 0), (0, DQK - LAT)))
        current = lax.dynamic_slice_in_dim(carried, start, span, 0)
        carried = lax.dynamic_update_slice_in_dim(carried, current + window_grad, start, 0)
        return carried, (attention, d_query)

    initial = jnp.zeros((reach * TOK_DEV + TOKENS, DQK), jnp.float32)
    summed, (attention, d_query) = lax.scan(one_block, initial, jnp.arange(block_count, dtype=jnp.int32))
    attention = attention.reshape(TOKENS, HEADS, LAT)
    d_query = d_query.reshape(TOKENS, HEADS, DQK)
    d_key = summed[reach * TOK_DEV:]
    return attention, d_query, d_key
```

```python
import jax
import jax.numpy as jnp
from jax import lax
from jax.experimental import pallas as pl
from jax.experimental.pallas import tpu as pltpu
from jax.sharding import PartitionSpec as P

MAXDOC = 256
SCALE = 192 ** (-0.5)
BF = jnp.bfloat16
F32 = jnp.float32
NT = (((1,), (1,)), ((), ()))
NN = (((1,), (0,)), ((), ()))
TN = (((0,), (0,)), ((), ()))


def dot(a, b, dims):
    return lax.dot_general(a, b, dims, preferred_element_type=F32)


def own_kernel(q_ref, g_ref, k_ref, gh_ref, s_ref, p_ref, wide):
    heads, lat = g_ref.shape[1], g_ref.shape[2]
    tok = g_ref.shape[0]
    for c in range(lat // 128):
        wide[c] = g_ref[:, :, c * 128 : (c + 1) * 128].astype(F32).reshape(tok * heads, 128)
    keys = k_ref[...].T
    for h in range(0, heads, 2):
        for i in (h, h + 1):
            for c in range(lat // 128):
                part = wide[c, pl.ds(i, tok, stride=heads), :]
                gh_ref[i * tok : (i + 1) * tok, c * 128 : (c + 1) * 128] = part.astype(BF)
        cols = slice(h * tok, (h + 2) * tok)
        qs = jnp.concatenate([q_ref[h], q_ref[h + 1]], axis=1)
        s_ref[:, cols] = dot(keys, qs, NN)
        p_ref[:, cols] = dot(keys[:, :lat], gh_ref[cols, :], NT)


def main_kernel(ctx_ref, q_ref, gh_ref, s_ref, p_ref, k2_ref, k1_ref, doc_ref, w_ref, ds_ref, a2_ref, a1_ref):
    heads = q_ref.shape[0]
    tok = q_ref.shape[2]
    lat = gh_ref.shape[1]
    keys = jnp.concatenate([k2_ref[...].T, k1_ref[...].T], axis=0)
    base = ctx_ref[0] * tok
    kpos = base - 2 * tok + lax.broadcasted_iota(jnp.int32, (3 * tok, 2 * tok), 0)
    qpos = base + (lax.broadcasted_iota(jnp.int32, (3 * tok, 2 * tok), 1) % tok)
    doc = jnp.concatenate([doc_ref[...], doc_ref[...]], axis=1)
    seen = (kpos >= doc) & (kpos <= qpos)
    for h in range(0, heads, 2):
        cols = slice(h * tok, (h + 2) * tok)
        qs = jnp.concatenate([q_ref[h], q_ref[h + 1]], axis=1)
        s = jnp.concatenate([dot(keys, qs, NN), s_ref[:, cols]], axis=0) * SCALE
        s = jnp.where(seen, s, -jnp.inf)
        top = jnp.max(s, axis=0, keepdims=True)
        e = jnp.exp(s - top)
        prob = e * (1.0 / jnp.sum(e, axis=0, keepdims=True))
        dp = jnp.concatenate([dot(keys[:, :lat], gh_ref[cols, :], NT), p_ref[:, cols]], axis=0)
        delta = jnp.sum(prob * dp, axis=0, keepdims=True)
        w_ref[:, cols] = prob.astype(BF)
        ds_ref[:, cols] = (SCALE * prob * (dp - delta)).astype(BF)
    partial_grad(w_ref, ds_ref, q_ref, gh_ref, 0, a2_ref)
    partial_grad(w_ref, ds_ref, q_ref, gh_ref, 1, a1_ref)


def partial_grad(w_ref, ds_ref, q_ref, gh_ref, block, out_ref):
    heads, _, tok = q_ref.shape
    lat = gh_ref.shape[1]
    rows = slice(block * tok, (block + 1) * tok)
    qs = jnp.concatenate([q_ref[h] for h in range(heads)], axis=1)
    score_part = dot(ds_ref[rows, :], qs, NT)
    value_part = dot(w_ref[rows, :], gh_ref[...], NN)
    out_ref[:, :lat] = (score_part[:, :lat] + value_part).astype(out_ref.dtype)
    out_ref[:, lat:] = score_part[:, lat:].astype(out_ref.dtype)


def last_kernel(w_ref, ds_ref, q_ref, gh_ref, o_ref):
    partial_grad(w_ref, ds_ref, q_ref, gh_ref, 2, o_ref)


def out_kernel(w_ref, ds_ref, k2_ref, k1_ref, k0_ref, att_ref, dq_ref, wide):
    heads = dq_ref.shape[0]
    tok = dq_ref.shape[2]
    lat = att_ref.shape[2]
    kt = jnp.concatenate([k2_ref[...], k1_ref[...], k0_ref[...]], axis=1)
    for h in range(0, heads, 2):
        cols = slice(h * tok, (h + 2) * tok)
        dq = dot(kt, ds_ref[:, cols], NN).astype(BF)
        dq_ref[h] = dq[:, :tok]
        dq_ref[h + 1] = dq[:, tok:]
        for i in (h, h + 1):
            att = dot(w_ref[:, i * tok : (i + 1) * tok].T, kt[:lat, :], NT)
            for c in range(lat // 128):
                wide[c, pl.ds(i, tok, stride=heads), :] = att[:, c * 128 : (c + 1) * 128]
    for c in range(lat // 128):
        att_ref[:, :, c * 128 : (c + 1) * 128] = wide[c].reshape(tok, heads, 128).astype(BF)


def ctx_pairs(step, ctx_count, head_count, row):
    pairs = []
    for source in range(ctx_count):
        target = source + step
        if 0 <= target < ctx_count:
            flip = source // row != target // row
            for head in range(head_count):
                pairs.append((source * head_count + head, target * head_count + (head ^ 1 if flip else head)))
    return pairs


def shards(query_heads, key_latent, doc_start, out_grad):
    tok, heads, width = query_heads.shape
    lat = out_grad.shape[2]
    ctx_count = lax.axis_size("ctx")
    head_count = lax.axis_size("head")
    both = ("ctx", "head")
    rows = tok * heads

    def shift(value, step):
        return lax.ppermute(value, both, ctx_pairs(step, ctx_count, head_count, 16))

    ctx_index = lax.axis_index("ctx").astype(jnp.int32)
    k2 = shift(key_latent, 2).T
    k1 = shift(key_latent, 1).T
    k0 = key_latent.T
    qt = jnp.transpose(query_heads, (1, 2, 0))
    vmem = pl.BlockSpec(memory_space=pltpu.VMEM)
    smem = pl.BlockSpec(memory_space=pltpu.SMEM)
    shape = jax.ShapeDtypeStruct
    gh, s0, p0 = pl.pallas_call(
        own_kernel,
        out_shape=(shape((rows, lat), BF), shape((tok, rows), F32), shape((tok, rows), F32)),
        in_specs=[vmem] * 3,
        out_specs=(vmem,) * 3,
        scratch_shapes=[pltpu.VMEM((lat // 128, rows, 128), F32)],
        name="own",
    )(qt, out_grad, k0)
    w, ds, a2, a1 = pl.pallas_call(
        main_kernel,
        out_shape=(
            shape((3 * tok, rows), BF),
            shape((3 * tok, rows), BF),
            shape((tok, width), BF),
            shape((tok, width), BF),
        ),
        in_specs=[smem] + [vmem] * 7,
        out_specs=(vmem,) * 4,
        name="main",
    )(ctx_index.reshape(1), qt, gh, s0, p0, k2, k1, doc_start.reshape(1, tok))
    r2 = shift(a2, -2)
    r1 = shift(a1, -1)
    own = pl.pallas_call(
        last_kernel, out_shape=shape((tok, width), F32), in_specs=[vmem] * 4, out_specs=vmem, name="last"
    )(w, ds, qt, gh)
    att, dq = pl.pallas_call(
        out_kernel,
        out_shape=(shape((tok, heads, lat), BF), shape((heads, width, tok), BF)),
        in_specs=[vmem] * 5,
        out_specs=(vmem,) * 2,
        scratch_shapes=[pltpu.VMEM((lat // 128, rows, 128), F32)],
        name="outs",
    )(w, ds, k2, k1, k0)
    owned = (own + r2.astype(F32) + r1.astype(F32)).astype(BF)
    fours = head_count // 2
    groups = [[2 * y + z for y in range(fours)] for z in range(2)]
    pieces = lax.all_to_all(
        owned.reshape(fours, tok // fours, width), "head", 0, 0, axis_index_groups=groups, tiled=True
    )
    halves = jnp.sum(pieces.astype(F32), axis=0).reshape(2, tok // head_count, width)
    z = lax.axis_index("head") % 2
    mine = jnp.where(z == 0, halves[0], halves[1])
    other = jnp.where(z == 0, halves[1], halves[0]).astype(BF)
    got = lax.ppermute(other, "head", [(i, i ^ 1) for i in range(head_count)])
    d_key = mine + got.astype(F32)
    return (att, jnp.transpose(dq, (2, 0, 1)), d_key)


def solution(mesh):
    return jax.shard_map(
        shards,
        mesh=mesh,
        in_specs=(P("ctx", "head", None), P("ctx", None), P("ctx"), P("ctx", "head", None)),
        out_specs=(P("ctx", "head", None), P("ctx", "head", None), P(("ctx", "head"), None)),
        check_vma=False,
    )
```

```python
import jax
import jax.numpy as jnp
from jax import lax
from jax.experimental import pallas as pl
from jax.experimental.pallas import tpu as pltpu
from jax.sharding import PartitionSpec as P

SCALE = 192 ** (-0.5)
BF = jnp.bfloat16
F32 = jnp.float32
NT = (((1,), (1,)), ((), ()))
NN = (((1,), (0,)), ((), ()))


def dot(a, b, dims):
    return lax.dot_general(a, b, dims, preferred_element_type=F32)


def own_kernel(q_ref, g_ref, k_ref, qv_ref, kv_ref, gh_ref, s_ref, p_ref, gbuf, wide, sems):
    heads, _, tok = qv_ref.shape
    lat = gh_ref.shape[1]
    parts = 4
    size = tok // parts
    g_copies = []
    for n in range(parts):
        piece = slice(n * size, (n + 1) * size)
        g_copies.append(pltpu.make_async_copy(g_ref.at[piece], gbuf.at[piece], sems.at[n]))
    q_copies = [pltpu.make_async_copy(q_ref.at[h], qv_ref.at[h], sems.at[parts + h]) for h in range(heads)]
    k_copy = pltpu.make_async_copy(k_ref, kv_ref, sems.at[parts + heads])
    for copy in [k_copy] + g_copies + q_copies:
        copy.start()
    k_copy.wait()
    keys = kv_ref[...].T
    for n in range(parts):
        g_copies[n].wait()
        piece = slice(n * size, (n + 1) * size)
        rows = slice(n * size * heads, (n + 1) * size * heads)
        for c in range(lat // 128):
            wide[c, rows, :] = gbuf[piece, :, c * 128 : (c + 1) * 128].astype(F32).reshape(size * heads, 128)
    for h in range(0, heads, 2):
        for i in (h, h + 1):
            for c in range(lat // 128):
                part = wide[c, pl.ds(i, tok, stride=heads), :]
                gh_ref[i * tok : (i + 1) * tok, c * 128 : (c + 1) * 128] = part.astype(BF)
            q_copies[i].wait()
        cols = slice(h * tok, (h + 2) * tok)
        qs = jnp.concatenate([qv_ref[h], qv_ref[h + 1]], axis=1)
        s_ref[:, cols] = dot(keys, qs, NN)
        p_ref[:, cols] = dot(keys[:, :lat], gh_ref[cols, :], NT)


def mid_kernel(q_ref, gh_ref, k_ref, s_ref, p_ref):
    heads, _, tok = q_ref.shape
    lat = gh_ref.shape[1]
    keys = k_ref[...].T
    for h in range(0, heads, 2):
        cols = slice(h * tok, (h + 2) * tok)
        qs = jnp.concatenate([q_ref[h], q_ref[h + 1]], axis=1)
        s_ref[:, cols] = dot(keys, qs, NN)
        p_ref[:, cols] = dot(keys[:, :lat], gh_ref[cols, :], NT)


def main_kernel(ctx_ref, q_ref, gh_ref, s0_ref, p0_ref, s1_ref, p1_ref, k2_ref, doc_ref, w_ref, ds_ref, a2_ref):
    heads, _, tok = q_ref.shape
    lat = gh_ref.shape[1]
    keys = k2_ref[...].T
    base = ctx_ref[0] * tok
    kpos = base - 2 * tok + lax.broadcasted_iota(jnp.int32, (3 * tok, 2 * tok), 0)
    qpos = base + (lax.broadcasted_iota(jnp.int32, (3 * tok, 2 * tok), 1) % tok)
    doc = jnp.concatenate([doc_ref[...], doc_ref[...]], axis=1)
    seen = (kpos >= doc) & (kpos <= qpos)
    for h in range(0, heads, 2):
        cols = slice(h * tok, (h + 2) * tok)
        qs = jnp.concatenate([q_ref[h], q_ref[h + 1]], axis=1)
        s = jnp.concatenate([dot(keys, qs, NN), s1_ref[:, cols], s0_ref[:, cols]], axis=0) * SCALE
        s = jnp.where(seen, s, -jnp.inf)
        top = jnp.max(s, axis=0, keepdims=True)
        e = jnp.exp(s - top)
        prob = e * (1.0 / jnp.sum(e, axis=0, keepdims=True))
        dp = jnp.concatenate([dot(keys[:, :lat], gh_ref[cols, :], NT), p1_ref[:, cols], p0_ref[:, cols]], axis=0)
        delta = jnp.sum(prob * dp, axis=0, keepdims=True)
        w_ref[:, cols] = prob.astype(BF)
        ds_ref[:, cols] = (SCALE * prob * (dp - delta)).astype(BF)
    partial_grad(w_ref, ds_ref, q_ref, gh_ref, 0, a2_ref)


def partial_grad(w_ref, ds_ref, q_ref, gh_ref, block, out_ref):
    heads, _, tok = q_ref.shape
    lat = gh_ref.shape[1]
    rows = slice(block * tok, (block + 1) * tok)
    qs = jnp.concatenate([q_ref[h] for h in range(heads)], axis=1)
    score_part = dot(ds_ref[rows, :], qs, NT)
    value_part = dot(w_ref[rows, :], gh_ref[...], NN)
    out_ref[:, :lat] = (score_part[:, :lat] + value_part).astype(out_ref.dtype)
    out_ref[:, lat:] = score_part[:, lat:].astype(out_ref.dtype)


def back_kernel(w_ref, ds_ref, q_ref, gh_ref, o_ref):
    partial_grad(w_ref, ds_ref, q_ref, gh_ref, 1, o_ref)


def last_kernel(w_ref, ds_ref, q_ref, gh_ref, o_ref):
    partial_grad(w_ref, ds_ref, q_ref, gh_ref, 2, o_ref)


def add_kernel(own_ref, r2_ref, r1_ref, o_ref):
    total = own_ref[...] + r2_ref[...].astype(F32) + r1_ref[...].astype(F32)
    o_ref[...] = total.reshape(o_ref.shape).astype(BF)


def out_kernel(w_ref, ds_ref, k2_ref, k1_ref, k0_ref, att_ref, dq_ref, wide):
    heads = dq_ref.shape[0]
    tok = dq_ref.shape[2]
    lat = att_ref.shape[2]
    kt = jnp.concatenate([k2_ref[...], k1_ref[...], k0_ref[...]], axis=1)
    for h in range(0, heads, 2):
        cols = slice(h * tok, (h + 2) * tok)
        dq = dot(kt, ds_ref[:, cols], NN).astype(BF)
        dq_ref[h] = dq[:, :tok]
        dq_ref[h + 1] = dq[:, tok:]
        for i in (h, h + 1):
            att = dot(w_ref[:, i * tok : (i + 1) * tok].T, kt[:lat, :], NT)
            for c in range(lat // 128):
                wide[c, pl.ds(i, tok, stride=heads), :] = att[:, c * 128 : (c + 1) * 128]
    for c in range(lat // 128):
        att_ref[:, :, c * 128 : (c + 1) * 128] = wide[c].reshape(tok, heads, 128).astype(BF)


def ctx_pairs(step, ctx_count, head_count, row):
    pairs = []
    for source in range(ctx_count):
        target = source + step
        if 0 <= target < ctx_count:
            flip = source // row != target // row
            for head in range(head_count):
                pairs.append((source * head_count + head, target * head_count + (head ^ 1 if flip else head)))
    return pairs


def step(query_heads, key_latent, doc_start, out_grad):
    tok, heads, width = query_heads.shape
    lat = out_grad.shape[2]
    ctx_count = lax.axis_size("ctx")
    head_count = lax.axis_size("head")
    both = ("ctx", "head")
    rows = tok * heads

    def shift(value, step):
        return lax.ppermute(value, both, ctx_pairs(step, ctx_count, head_count, 16))

    ctx_index = lax.axis_index("ctx").astype(jnp.int32)
    k2 = shift(key_latent, 2).T
    k1 = shift(key_latent, 1).T
    k0 = key_latent.T
    qt = jnp.transpose(query_heads, (1, 2, 0))
    k2, k1 = (pltpu.with_memory_space_constraint(x, pltpu.VMEM) for x in (k2, k1))
    qt, out_grad, k0 = (pltpu.with_memory_space_constraint(x, pltpu.HBM) for x in (qt, out_grad, k0))
    vmem = pl.BlockSpec(memory_space=pltpu.VMEM)
    smem = pl.BlockSpec(memory_space=pltpu.SMEM)
    shape = jax.ShapeDtypeStruct
    hbm = pl.BlockSpec(memory_space=pltpu.HBM)
    qv, kv, gh, s0, p0 = pl.pallas_call(
        own_kernel,
        out_shape=(pltpu.VMEM((heads, width, tok), BF), pltpu.VMEM((width, tok), BF), pltpu.VMEM((rows, lat), BF), pltpu.VMEM((tok, rows), F32), pltpu.VMEM((tok, rows), F32)),
        in_specs=[hbm] * 3,
        out_specs=(vmem,) * 5,
        scratch_shapes=[
            pltpu.VMEM((tok, heads, lat), BF),
            pltpu.VMEM((lat // 128, rows, 128), F32),
            pltpu.SemaphoreType.DMA((5 + heads,)),
        ],
        compiler_params=pltpu.CompilerParams(vmem_limit_bytes=16 << 20), name="own",
    )(qt, out_grad, k0)
    params = pltpu.CompilerParams(vmem_limit_bytes=16 << 20)
    s1, p1 = pl.pallas_call(
        mid_kernel,
        out_shape=(pltpu.VMEM((tok, rows), F32), pltpu.VMEM((tok, rows), F32)),
        in_specs=[vmem] * 3,
        out_specs=(vmem,) * 2,
        compiler_params=params,
        name="mid",
    )(qv, gh, k1)
    w, ds, a2 = pl.pallas_call(
        main_kernel,
        out_shape=(
            pltpu.VMEM((3 * tok, rows), BF),
            pltpu.VMEM((3 * tok, rows), BF),
            pltpu.VMEM((tok, width), BF),
        ),
        in_specs=[smem] + [vmem] * 8,
        out_specs=(vmem,) * 3,
        compiler_params=params,
        name="main",
    )(ctx_index.reshape(1), qv, gh, s0, p0, s1, p1, k2, doc_start.reshape(1, tok))
    r2 = shift(a2, -2)
    a1 = pl.pallas_call(
        back_kernel,
        out_shape=pltpu.VMEM((tok, width), BF),
        in_specs=[vmem] * 4,
        out_specs=vmem,
        compiler_params=params,
        name="back",
    )(w, ds, qv, gh)
    r1 = shift(a1, -1)
    own = pl.pallas_call(
        last_kernel, out_shape=pltpu.VMEM((tok, width), F32), in_specs=[vmem] * 4, out_specs=vmem, compiler_params=pltpu.CompilerParams(vmem_limit_bytes=16 << 20), name="last"
    )(w, ds, qv, gh)
    att, dq = pl.pallas_call(
        out_kernel,
        out_shape=(shape((tok, heads, lat), BF), shape((heads, width, tok), BF)),
        in_specs=[vmem] * 5,
        out_specs=(vmem,) * 2,
        scratch_shapes=[pltpu.VMEM((lat // 128, rows, 128), F32)],
        compiler_params=pltpu.CompilerParams(vmem_limit_bytes=16 << 20), name="outs",
    )(w, ds, k2, k1, kv)
    r2, r1 = (pltpu.with_memory_space_constraint(x, pltpu.VMEM) for x in (r2, r1))
    fours = head_count // 2
    owned = pl.pallas_call(
        add_kernel,
        out_shape=pltpu.VMEM((fours, tok // fours, width), BF),
        in_specs=[vmem] * 3,
        out_specs=vmem,
        compiler_params=pltpu.CompilerParams(vmem_limit_bytes=16 << 20),
        name="add",
    )(own, r2, r1)
    groups = [[2 * y + z for y in range(fours)] for z in range(2)]
    pieces = lax.all_to_all(
        owned, "head", 0, 0, axis_index_groups=groups, tiled=True
    )
    halves = jnp.sum(pieces.astype(F32), axis=0).reshape(2, tok // head_count, width)
    z = lax.axis_index("head") % 2
    mine = jnp.where(z == 0, halves[0], halves[1])
    other = jnp.where(z == 0, halves[1], halves[0]).astype(BF)
    pairs = [[2 * y, 2 * y + 1] for y in range(fours)]
    got = lax.all_gather(other, "head", axis_index_groups=pairs)
    d_key = mine + jnp.where(z == 0, got[1], got[0]).astype(F32)
    return (att, jnp.transpose(dq, (2, 0, 1)), d_key)


def solution(mesh):
    return jax.shard_map(
        step,
        mesh=mesh,
        in_specs=(P("ctx", "head", None), P("ctx", None), P("ctx"), P("ctx", "head", None)),
        out_specs=(P("ctx", "head", None), P("ctx", "head", None), P(("ctx", "head"), None)),
        check_vma=False,
    )
```

```python
import jax
import jax.numpy as jnp
from jax import lax
from jax.experimental import pallas as pl
from jax.experimental.pallas import tpu as pltpu
from jax.sharding import PartitionSpec as P

SCALE = 192 ** (-0.5)
LANES = 128
BF = jnp.bfloat16
F32 = jnp.float32
NT = (((1,), (1,)), ((), ()))
NN = (((1,), (0,)), ((), ()))


def dot(a, b, dims):
    return lax.dot_general(a, b, dims, preferred_element_type=F32)


def two_heads(q_ref, h):
    return jnp.concatenate([q_ref[h], q_ref[h + 1]], axis=1)


def own_kernel(q_ref, g_ref, k_ref, qv_ref, kv_ref, gh_ref, s_ref, p_ref, gbuf, wide, sems):
    heads, _, tok = qv_ref.shape
    lat = gh_ref.shape[1]
    parts = 4
    size = tok // parts
    g_copies = []
    for n in range(parts):
        piece = slice(n * size, (n + 1) * size)
        g_copies.append(pltpu.make_async_copy(g_ref.at[piece], gbuf.at[piece], sems.at[n]))
    q_copies = [pltpu.make_async_copy(q_ref.at[h], qv_ref.at[h], sems.at[parts + h]) for h in range(heads)]
    k_copy = pltpu.make_async_copy(k_ref, kv_ref, sems.at[parts + heads])
    for copy in [k_copy] + g_copies + q_copies:
        copy.start()
    k_copy.wait()
    keys = kv_ref[...].T
    for n in range(parts):
        g_copies[n].wait()
        piece = slice(n * size, (n + 1) * size)
        rows = slice(n * size * heads, (n + 1) * size * heads)
        for c in range(lat // LANES):
            lanes = slice(c * LANES, (c + 1) * LANES)
            wide[c, rows, :] = gbuf[piece, :, lanes].astype(F32).reshape(size * heads, LANES)
    for h in range(0, heads, 2):
        for i in (h, h + 1):
            for c in range(lat // LANES):
                part = wide[c, pl.ds(i, tok, stride=heads), :]
                gh_ref[i * tok : (i + 1) * tok, c * LANES : (c + 1) * LANES] = part.astype(BF)
            q_copies[i].wait()
        cols = slice(h * tok, (h + 2) * tok)
        s_ref[:, cols] = dot(keys, two_heads(qv_ref, h), NN)
        p_ref[:, cols] = dot(keys[:, :lat], gh_ref[cols, :], NT)


def visible(ctx_ref, doc_ref, back, blocks):
    tok = doc_ref.shape[1]
    base = ctx_ref[0] * tok
    dims = (blocks * tok, 2 * tok)
    kpos = base - back * tok + lax.broadcasted_iota(jnp.int32, dims, 0)
    qpos = base + (lax.broadcasted_iota(jnp.int32, dims, 1) % tok)
    doc = jnp.concatenate([doc_ref[...], doc_ref[...]], axis=1)
    return (kpos >= doc) & (kpos <= qpos)


def mid_kernel(ctx_ref, q_ref, gh_ref, s0_ref, p0_ref, k_ref, doc_ref, e_ref, p_ref, top_ref, sum_ref, del_ref):
    heads, _, tok = q_ref.shape
    lat = gh_ref.shape[1]
    keys = k_ref[...].T
    seen = visible(ctx_ref, doc_ref, 1, 2)
    for h in range(0, heads, 2):
        cols = slice(h * tok, (h + 2) * tok)
        s = jnp.concatenate([dot(keys, two_heads(q_ref, h), NN), s0_ref[:, cols]], axis=0) * SCALE
        s = jnp.where(seen, s, -jnp.inf)
        top = jnp.max(s, axis=0, keepdims=True)
        e = jnp.exp(s - top)
        p1 = dot(keys[:, :lat], gh_ref[cols, :], NT)
        dp = jnp.concatenate([p1, p0_ref[:, cols]], axis=0)
        e_ref[:, cols] = e
        p_ref[:, cols] = p1
        top_ref[:, cols] = top
        sum_ref[:, cols] = jnp.sum(e, axis=0, keepdims=True)
        del_ref[:, cols] = jnp.sum(e * dp, axis=0, keepdims=True)


def main_kernel(
    ctx_ref, q_ref, gh_ref, top_ref, sum_ref, del_ref, k2_ref, doc_ref, w_ref, ds_ref, fac_ref, delta_ref, a2_ref
):
    heads, _, tok = q_ref.shape
    lat = gh_ref.shape[1]
    keys = k2_ref[...].T
    seen = visible(ctx_ref, doc_ref, 2, 1)
    for h in range(0, heads, 2):
        cols = slice(h * tok, (h + 2) * tok)
        s = jnp.where(seen, dot(keys, two_heads(q_ref, h), NN) * SCALE, -jnp.inf)
        before = top_ref[:, cols]
        top = jnp.maximum(before, jnp.max(s, axis=0, keepdims=True))
        e = jnp.exp(s - top)
        old = jnp.exp(before - top)
        inv = 1.0 / (old * sum_ref[:, cols] + jnp.sum(e, axis=0, keepdims=True))
        dp = dot(keys[:, :lat], gh_ref[cols, :], NT)
        delta = (old * del_ref[:, cols] + jnp.sum(e * dp, axis=0, keepdims=True)) * inv
        prob = e * inv
        w_ref[:, cols] = prob.astype(BF)
        ds_ref[:, cols] = (SCALE * prob * (dp - delta)).astype(BF)
        fac_ref[:, cols] = old * inv
        delta_ref[:, cols] = delta
    put_packed(partial_grad(w_ref, ds_ref, q_ref, gh_ref), a2_ref, lat)


def partial_grad(w_ref, ds_ref, q_ref, gh_ref):
    heads = q_ref.shape[0]
    lat = gh_ref.shape[1]
    qs = jnp.concatenate([q_ref[h] for h in range(heads)], axis=1)
    score_part = dot(ds_ref[...], qs, NT)
    value_part = dot(w_ref[...], gh_ref[...], NN)
    return score_part[:, :lat] + value_part, score_part[:, lat:]


def put_packed(parts, out_ref, lat):
    main, rest = parts
    tok, width = rest.shape
    fold = LANES // width
    rows = tok // fold
    rest = jnp.concatenate([rest[n * rows : (n + 1) * rows] for n in range(fold)], axis=1)
    count = lat // LANES
    out_ref[:tok, :] = main.astype(BF)
    for n in range(count):
        piece = rest[n * rows // count : (n + 1) * rows // count]
        out_ref[tok:, n * LANES : (n + 1) * LANES] = piece.astype(BF)


def get_packed(ref, tok, width):
    lat = ref.shape[1]
    rest = ref[tok:, :].astype(F32)
    rest = jnp.concatenate([rest[:, n * LANES : (n + 1) * LANES] for n in range(lat // LANES)], axis=0)
    rest = jnp.concatenate([rest[:, n * width : (n + 1) * width] for n in range(LANES // width)], axis=0)
    return ref[:tok, :].astype(F32), rest


def finish(e_ref, p_ref, fac_ref, delta_ref, block, w_ref, ds_ref):
    tok = w_ref.shape[0]
    prob = e_ref[block * tok : (block + 1) * tok, :] * fac_ref[...]
    w_ref[...] = prob.astype(BF)
    ds_ref[...] = (SCALE * prob * (p_ref[...] - delta_ref[...])).astype(BF)


def back_kernel(e_ref, p_ref, fac_ref, delta_ref, q_ref, gh_ref, w_ref, ds_ref, o_ref):
    finish(e_ref, p_ref, fac_ref, delta_ref, 0, w_ref, ds_ref)
    put_packed(partial_grad(w_ref, ds_ref, q_ref, gh_ref), o_ref, gh_ref.shape[1])


def last_kernel(e_ref, p_ref, fac_ref, delta_ref, q_ref, gh_ref, w_ref, ds_ref, o_ref):
    lat = gh_ref.shape[1]
    finish(e_ref, p_ref, fac_ref, delta_ref, 1, w_ref, ds_ref)
    main, rest = partial_grad(w_ref, ds_ref, q_ref, gh_ref)
    o_ref[:, :lat] = main
    o_ref[:, lat:] = rest


def add_kernel(own_ref, r2_ref, r1_ref, o_ref):
    tok, width = own_ref.shape
    lat = r2_ref.shape[1]
    main2, rest2 = get_packed(r2_ref, tok, width - lat)
    main1, rest1 = get_packed(r1_ref, tok, width - lat)
    dims = o_ref.shape[:2]
    o_ref[:, :, :lat] = (own_ref[:, :lat] + main2 + main1).reshape(*dims, lat).astype(BF)
    o_ref[:, :, lat:] = (own_ref[:, lat:] + rest2 + rest1).reshape(*dims, width - lat).astype(BF)


def att_kernel(w2_ref, w1_ref, w0_ref, k2_ref, k1_ref, k0_ref, att_ref, wide):
    tok, heads, lat = att_ref.shape
    kt = jnp.concatenate([k2_ref[:lat], k1_ref[:lat], k0_ref[:lat]], axis=1)
    for i in range(heads):
        cols = slice(i * tok, (i + 1) * tok)
        weights = jnp.concatenate([w2_ref[:, cols].T, w1_ref[:, cols].T, w0_ref[:, cols].T], axis=1)
        att = dot(weights, kt, NT)
        for c in range(lat // LANES):
            wide[c, pl.ds(i, tok, stride=heads), :] = att[:, c * LANES : (c + 1) * LANES]
    for c in range(lat // LANES):
        att_ref[:, :, c * LANES : (c + 1) * LANES] = wide[c].reshape(tok, heads, LANES).astype(BF)


def dq_kernel(ds2_ref, ds1_ref, ds0_ref, k2_ref, k1_ref, k0_ref, dq_ref):
    heads, _, tok = dq_ref.shape
    kt = jnp.concatenate([k2_ref[...], k1_ref[...], k0_ref[...]], axis=1)
    for h in range(0, heads, 2):
        cols = slice(h * tok, (h + 2) * tok)
        ds = jnp.concatenate([ds2_ref[:, cols], ds1_ref[:, cols], ds0_ref[:, cols]], axis=0)
        dq = dot(kt, ds, NN).astype(BF)
        dq_ref[h] = dq[:, :tok]
        dq_ref[h + 1] = dq[:, tok:]


def ctx_pairs(step, ctx_count, head_count, row):
    pairs = []
    for source in range(ctx_count):
        target = source + step
        if 0 <= target < ctx_count:
            flip = source // row != target // row
            for head in range(head_count):
                pairs.append((source * head_count + head, target * head_count + (head ^ 1 if flip else head)))
    return pairs


def in_vmem(*values):
    return tuple(pltpu.with_memory_space_constraint(x, pltpu.VMEM) for x in values)


def call(kernel, out, ins, scratch=()):
    vmem = pl.BlockSpec(memory_space=pltpu.VMEM)
    specs = {"smem": pl.BlockSpec(memory_space=pltpu.SMEM), "hbm": pl.BlockSpec(memory_space=pltpu.HBM)}
    return pl.pallas_call(
        kernel,
        out_shape=out,
        in_specs=[specs.get(where, vmem) for where, _ in ins],
        out_specs=jax.tree.map(lambda _: vmem, out),
        scratch_shapes=scratch,
        compiler_params=pltpu.CompilerParams(vmem_limit_bytes=16 << 20),
    )(*[value for _, value in ins])


def v(*values):
    return [("vmem", value) for value in values]


def step(query_heads, key_latent, doc_start, out_grad):
    tok, heads, width = query_heads.shape
    lat = out_grad.shape[2]
    ctx_count = lax.axis_size("ctx")
    head_count = lax.axis_size("head")
    both = ("ctx", "head")
    rows = tok * heads
    packed = (tok * width // lat, lat)
    mem = pltpu.VMEM
    shape = jax.ShapeDtypeStruct

    def shift(value, steps):
        return lax.ppermute(value, both, ctx_pairs(steps, ctx_count, head_count, 16))

    ctx = ("smem", lax.axis_index("ctx").astype(jnp.int32).reshape(1))
    doc = doc_start.reshape(1, tok)
    kt = key_latent.T
    k1 = shift(kt, 1)
    k2 = shift(kt, 2)
    k2, k1 = in_vmem(k2, k1)
    qt = jnp.transpose(query_heads, (1, 2, 0))
    qt, og, kt = (pltpu.with_memory_space_constraint(x, pltpu.HBM) for x in (qt, out_grad, kt))
    wide_buf = mem((lat // LANES, rows, LANES), F32)
    qv, k0, gh, s0, p0 = call(
        own_kernel,
        (
            mem((heads, width, tok), BF),
            mem((width, tok), BF),
            mem((rows, lat), BF),
            mem((tok, rows), F32),
            mem((tok, rows), F32),
        ),
        [("hbm", qt), ("hbm", og), ("hbm", kt)],
        (mem((tok, heads, lat), BF), wide_buf, pltpu.SemaphoreType.DMA((5 + heads,))),
    )
    row = mem((1, rows), F32)
    e, p1, top, total, part = call(
        mid_kernel,
        (mem((2 * tok, rows), F32), mem((tok, rows), F32), row, row, row),
        [ctx] + v(qv, gh, s0, p0, k1, doc),
    )
    tile = mem((tok, rows), BF)
    w2, ds2, fac, delta, a2 = call(
        main_kernel, (tile, tile, row, row, mem(packed, BF)), [ctx] + v(qv, gh, top, total, part, k2, doc)
    )
    r2 = shift(a2, -2)
    w1, ds1, a1 = call(back_kernel, (tile, tile, mem(packed, BF)), v(e, p1, fac, delta, qv, gh))
    r1 = shift(a1, -1)
    w0, ds0, own = call(last_kernel, (tile, tile, mem((tok, width), F32)), v(e, p0, fac, delta, qv, gh))
    att = call(att_kernel, shape((tok, heads, lat), BF), v(w2, w1, w0, k2, k1, k0), (wide_buf,))
    dq = call(dq_kernel, shape((heads, width, tok), BF), v(ds2, ds1, ds0, k2, k1, k0))
    r2, r1 = in_vmem(r2, r1)
    fours = head_count // 2
    owned = call(add_kernel, mem((fours, tok // fours, width), BF), v(own, r2, r1))
    groups = [[2 * y + z for y in range(fours)] for z in range(2)]
    pieces = lax.all_to_all(owned, "head", 0, 0, axis_index_groups=groups, tiled=True)
    halves = jnp.sum(pieces.astype(F32), axis=0).reshape(2, tok // head_count, width)
    z = lax.axis_index("head") % 2
    mine = jnp.where(z == 0, halves[0], halves[1])
    other = jnp.where(z == 0, halves[1], halves[0]).astype(BF)
    pairs = [[2 * y, 2 * y + 1] for y in range(fours)]
    got = lax.all_gather(other, "head", axis_index_groups=pairs)
    d_key = mine + jnp.where(z == 0, got[1], got[0]).astype(F32)
    return (att, jnp.transpose(dq, (2, 0, 1)), d_key)


def solution(mesh):
    return jax.shard_map(
        step,
        mesh=mesh,
        in_specs=(P("ctx", "head", None), P("ctx", None), P("ctx"), P("ctx", "head", None)),
        out_specs=(P("ctx", "head", None), P("ctx", "head", None), P(("ctx", "head"), None)),
        check_vma=False,
    )
```

```python
import jax
import jax.numpy as jnp
from jax import lax
from jax.experimental import pallas as pl
from jax.experimental.pallas import tpu as pltpu
from jax.sharding import PartitionSpec as P

SCALE = 192 ** (-0.5)
LANES = 128
BF = jnp.bfloat16
F32 = jnp.float32
NT = (((1,), (1,)), ((), ()))
NN = (((1,), (0,)), ((), ()))


def dot(a, b, dims):
    return lax.dot_general(a, b, dims, preferred_element_type=F32)


def two_heads(q_ref, h):
    return jnp.concatenate([q_ref[h], q_ref[h + 1]], axis=1)


def own_kernel(q_ref, g_ref, k_ref, qv_ref, kv_ref, gh_ref, s_ref, p_ref, gbuf, wide, sems):
    heads, _, tok = qv_ref.shape
    lat = gh_ref.shape[1]
    parts = 4
    size = tok // parts
    g_copies = []
    for n in range(parts):
        piece = slice(n * size, (n + 1) * size)
        g_copies.append(pltpu.make_async_copy(g_ref.at[piece], gbuf.at[piece], sems.at[n]))
    q_copies = [pltpu.make_async_copy(q_ref.at[h], qv_ref.at[h], sems.at[parts + h]) for h in range(heads)]
    k_copy = pltpu.make_async_copy(k_ref, kv_ref, sems.at[parts + heads])
    for copy in [k_copy] + g_copies + q_copies:
        copy.start()
    k_copy.wait()
    keys = kv_ref[...].T
    for n in range(parts):
        g_copies[n].wait()
        piece = slice(n * size, (n + 1) * size)
        rows = slice(n * size * heads, (n + 1) * size * heads)
        for c in range(lat // LANES):
            lanes = slice(c * LANES, (c + 1) * LANES)
            wide[c, rows, :] = gbuf[piece, :, lanes].astype(F32).reshape(size * heads, LANES)
    for h in range(0, heads, 2):
        for i in (h, h + 1):
            for c in range(lat // LANES):
                part = wide[c, pl.ds(i, tok, stride=heads), :]
                gh_ref[i * tok : (i + 1) * tok, c * LANES : (c + 1) * LANES] = part.astype(BF)
            q_copies[i].wait()
        cols = slice(h * tok, (h + 2) * tok)
        s_ref[:, cols] = dot(keys, two_heads(qv_ref, h), NN)
        p_ref[:, cols] = dot(keys[:, :lat], gh_ref[cols, :], NT)


def visible(ctx_ref, doc_ref, blocks):
    tok = doc_ref.shape[1]
    base = ctx_ref[0] * tok
    row = lax.broadcasted_iota(jnp.int32, (tok, 2 * tok), 0)
    qpos = base + (lax.broadcasted_iota(jnp.int32, (tok, 2 * tok), 1) % tok)
    doc = jnp.concatenate([doc_ref[...], doc_ref[...]], axis=1)
    seen = [(base - back * tok + row >= doc) & (base - back * tok + row <= qpos) for back in blocks]
    return seen


def mid_kernel(ctx_ref, q_ref, gh_ref, s0_ref, p0_ref, k_ref, doc_ref, e_ref, p_ref, top_ref, sum_ref, del_ref):
    heads, _, tok = q_ref.shape
    lat = gh_ref.shape[1]
    keys = k_ref[...].T
    seen = visible(ctx_ref, doc_ref, (2, 0))
    for h in range(0, heads, 2):
        cols = slice(h * tok, (h + 2) * tok)
        far = jnp.where(seen[0], dot(keys, two_heads(q_ref, h), NN) * SCALE, -jnp.inf)
        own = jnp.where(seen[1], s0_ref[:, cols] * SCALE, -jnp.inf)
        s = jnp.concatenate([far, own], axis=0)
        top = jnp.max(s, axis=0, keepdims=True)
        e = jnp.exp(s - top)
        p1 = dot(keys[:, :lat], gh_ref[cols, :], NT)
        dp = jnp.concatenate([p1, p0_ref[:, cols]], axis=0)
        e_ref[:, cols] = e
        p_ref[:, cols] = p1
        top_ref[:, cols] = top
        sum_ref[:, cols] = jnp.sum(e, axis=0, keepdims=True)
        del_ref[:, cols] = jnp.sum(e * dp, axis=0, keepdims=True)


def main_kernel(
    ctx_ref, q_ref, gh_ref, e_ref, p2_ref, top_ref, sum_ref, del_ref, k1_ref, doc_ref, *outs
):
    w2_ref, ds2_ref, w_ref, ds_ref, fac_ref, delta_ref, a2_ref, a1_ref = outs
    heads, _, tok = q_ref.shape
    lat = gh_ref.shape[1]
    keys = k1_ref[...].T
    (seen,) = visible(ctx_ref, doc_ref, (1,))
    for h in range(0, heads, 2):
        cols = slice(h * tok, (h + 2) * tok)
        s = jnp.where(seen, dot(keys, two_heads(q_ref, h), NN) * SCALE, -jnp.inf)
        before = top_ref[:, cols]
        top = jnp.maximum(before, jnp.max(s, axis=0, keepdims=True))
        e = jnp.exp(s - top)
        old = jnp.exp(before - top)
        inv = 1.0 / (old * sum_ref[:, cols] + jnp.sum(e, axis=0, keepdims=True))
        dp = dot(keys[:, :lat], gh_ref[cols, :], NT)
        delta = (old * del_ref[:, cols] + jnp.sum(e * dp, axis=0, keepdims=True)) * inv
        prob = e * inv
        w_ref[:, cols] = prob.astype(BF)
        ds_ref[:, cols] = (SCALE * prob * (dp - delta)).astype(BF)
        fac_ref[:, cols] = old * inv
        delta_ref[:, cols] = delta
        prob = e_ref[:tok, cols] * (old * inv)
        w2_ref[:, cols] = prob.astype(BF)
        ds2_ref[:, cols] = (SCALE * prob * (p2_ref[:, cols] - delta)).astype(BF)
    put_packed(partial_grad(w2_ref, ds2_ref, q_ref, gh_ref), a2_ref, lat)
    put_packed(partial_grad(w_ref, ds_ref, q_ref, gh_ref), a1_ref, lat)


def partial_grad(w_ref, ds_ref, q_ref, gh_ref):
    heads = q_ref.shape[0]
    lat = gh_ref.shape[1]
    qs = jnp.concatenate([q_ref[h] for h in range(heads)], axis=1)
    score_part = dot(ds_ref[...], qs, NT)
    value_part = dot(w_ref[...], gh_ref[...], NN)
    return score_part[:, :lat] + value_part, score_part[:, lat:]


def put_packed(parts, out_ref, lat):
    main, rest = parts
    tok, width = rest.shape
    fold = LANES // width
    rows = tok // fold
    rest = jnp.concatenate([rest[n * rows : (n + 1) * rows] for n in range(fold)], axis=1)
    count = lat // LANES
    out_ref[:tok, :] = main.astype(BF)
    for n in range(count):
        piece = rest[n * rows // count : (n + 1) * rows // count]
        out_ref[tok:, n * LANES : (n + 1) * LANES] = piece.astype(BF)


def get_packed(ref, tok, width):
    lat = ref.shape[1]
    rest = ref[tok:, :].astype(F32)
    rest = jnp.concatenate([rest[:, n * LANES : (n + 1) * LANES] for n in range(lat // LANES)], axis=0)
    rest = jnp.concatenate([rest[:, n * width : (n + 1) * width] for n in range(LANES // width)], axis=0)
    return ref[:tok, :].astype(F32), rest


def last_kernel(e_ref, p_ref, fac_ref, delta_ref, q_ref, gh_ref, w_ref, ds_ref, o_ref):
    lat = gh_ref.shape[1]
    tok = w_ref.shape[0]
    prob = e_ref[tok:, :] * fac_ref[...]
    w_ref[...] = prob.astype(BF)
    ds_ref[...] = (SCALE * prob * (p_ref[...] - delta_ref[...])).astype(BF)
    main, rest = partial_grad(w_ref, ds_ref, q_ref, gh_ref)
    o_ref[:, :lat] = main
    o_ref[:, lat:] = rest


def add_kernel(own_ref, r2_ref, r1_ref, o_ref):
    tok, width = own_ref.shape
    lat = r2_ref.shape[1]
    main2, rest2 = get_packed(r2_ref, tok, width - lat)
    main1, rest1 = get_packed(r1_ref, tok, width - lat)
    dims = o_ref.shape[:2]
    o_ref[:, :, :lat] = (own_ref[:, :lat] + main2 + main1).reshape(*dims, lat).astype(BF)
    o_ref[:, :, lat:] = (own_ref[:, lat:] + rest2 + rest1).reshape(*dims, width - lat).astype(BF)


def att_kernel(w2_ref, w1_ref, w0_ref, k2_ref, k1_ref, k0_ref, att_ref, wide):
    tok, heads, lat = att_ref.shape
    kt = jnp.concatenate([k2_ref[:lat], k1_ref[:lat], k0_ref[:lat]], axis=1)
    for i in range(heads):
        cols = slice(i * tok, (i + 1) * tok)
        weights = jnp.concatenate([w2_ref[:, cols].T, w1_ref[:, cols].T, w0_ref[:, cols].T], axis=1)
        att = dot(weights, kt, NT)
        for c in range(lat // LANES):
            wide[c, pl.ds(i, tok, stride=heads), :] = att[:, c * LANES : (c + 1) * LANES]
    for c in range(lat // LANES):
        att_ref[:, :, c * LANES : (c + 1) * LANES] = wide[c].reshape(tok, heads, LANES).astype(BF)


def dq_kernel(ds2_ref, ds1_ref, ds0_ref, k2_ref, k1_ref, k0_ref, dq_ref):
    heads, _, tok = dq_ref.shape
    kt = jnp.concatenate([k2_ref[...], k1_ref[...], k0_ref[...]], axis=1)
    for h in range(0, heads, 2):
        cols = slice(h * tok, (h + 2) * tok)
        ds = jnp.concatenate([ds2_ref[:, cols], ds1_ref[:, cols], ds0_ref[:, cols]], axis=0)
        dq = dot(kt, ds, NN).astype(BF)
        dq_ref[h] = dq[:, :tok]
        dq_ref[h + 1] = dq[:, tok:]


def ctx_pairs(step, ctx_count, head_count, row):
    pairs = []
    for source in range(ctx_count):
        target = source + step
        if 0 <= target < ctx_count:
            flip = source // row != target // row
            for head in range(head_count):
                pairs.append((source * head_count + head, target * head_count + (head ^ 1 if flip else head)))
    return pairs


def in_vmem(*values):
    return tuple(pltpu.with_memory_space_constraint(x, pltpu.VMEM) for x in values)


def call(kernel, out, ins, scratch=()):
    vmem = pl.BlockSpec(memory_space=pltpu.VMEM)
    specs = {"smem": pl.BlockSpec(memory_space=pltpu.SMEM), "hbm": pl.BlockSpec(memory_space=pltpu.HBM)}
    return pl.pallas_call(
        kernel,
        out_shape=out,
        in_specs=[specs.get(where, vmem) for where, _ in ins],
        out_specs=jax.tree.map(lambda _: vmem, out),
        scratch_shapes=scratch,
        compiler_params=pltpu.CompilerParams(vmem_limit_bytes=16 << 20),
    )(*[value for _, value in ins])


def v(*values):
    return [("vmem", value) for value in values]


def step(query_heads, key_latent, doc_start, out_grad):
    tok, heads, width = query_heads.shape
    lat = out_grad.shape[2]
    ctx_count = lax.axis_size("ctx")
    head_count = lax.axis_size("head")
    both = ("ctx", "head")
    rows = tok * heads
    packed = (tok * width // lat, lat)
    mem = pltpu.VMEM
    shape = jax.ShapeDtypeStruct

    def shift(value, steps):
        return lax.ppermute(value, both, ctx_pairs(steps, ctx_count, head_count, 16))

    ctx = ("smem", lax.axis_index("ctx").astype(jnp.int32).reshape(1))
    doc = doc_start.reshape(1, tok)
    kt = key_latent.T
    k2 = shift(kt, 2)
    k1 = shift(kt, 1)
    k2, k1 = in_vmem(k2, k1)
    qt = jnp.transpose(query_heads, (1, 2, 0))
    qt, og, kt = (pltpu.with_memory_space_constraint(x, pltpu.HBM) for x in (qt, out_grad, kt))
    wide_buf = mem((lat // LANES, rows, LANES), F32)
    qv, k0, gh, s0, p0 = call(
        own_kernel,
        (
            mem((heads, width, tok), BF),
            mem((width, tok), BF),
            mem((rows, lat), BF),
            mem((tok, rows), F32),
            mem((tok, rows), F32),
        ),
        [("hbm", qt), ("hbm", og), ("hbm", kt)],
        (mem((tok, heads, lat), BF), wide_buf, pltpu.SemaphoreType.DMA((5 + heads,))),
    )
    row = mem((1, rows), F32)
    e, p2, top, total, part = call(
        mid_kernel,
        (mem((2 * tok, rows), F32), mem((tok, rows), F32), row, row, row),
        [ctx] + v(qv, gh, s0, p0, k2, doc),
    )
    tile = mem((tok, rows), BF)
    w2, ds2, w1, ds1, fac, delta, a2, a1 = call(
        main_kernel,
        (tile, tile, tile, tile, row, row, mem(packed, BF), mem(packed, BF)),
        [ctx] + v(qv, gh, e, p2, top, total, part, k1, doc),
    )
    r2 = shift(a2, -2)
    r1 = shift(a1, -1)
    w0, ds0, own = call(last_kernel, (tile, tile, mem((tok, width), F32)), v(e, p0, fac, delta, qv, gh))
    att = call(att_kernel, shape((tok, heads, lat), BF), v(w2, w1, w0, k2, k1, k0), (wide_buf,))
    dq = call(dq_kernel, shape((heads, width, tok), BF), v(ds2, ds1, ds0, k2, k1, k0))
    r2, r1 = in_vmem(r2, r1)
    fours = head_count // 2
    owned = call(add_kernel, mem((fours, tok // fours, width), BF), v(own, r2, r1))
    groups = [[2 * y + z for y in range(fours)] for z in range(2)]
    pieces = lax.all_to_all(owned, "head", 0, 0, axis_index_groups=groups, tiled=True)
    halves = jnp.sum(pieces.astype(F32), axis=0).reshape(2, tok // head_count, width)
    z = lax.axis_index("head") % 2
    mine = jnp.where(z == 0, halves[0], halves[1])
    other = jnp.where(z == 0, halves[1], halves[0]).astype(BF)
    pairs = [[2 * y, 2 * y + 1] for y in range(fours)]
    got = lax.all_gather(other, "head", axis_index_groups=pairs)
    d_key = mine + jnp.where(z == 0, got[1], got[0]).astype(F32)
    return (att, jnp.transpose(dq, (2, 0, 1)), d_key)


def solution(mesh):
    return jax.shard_map(
        step,
        mesh=mesh,
        in_specs=(P("ctx", "head", None), P("ctx", None), P("ctx"), P("ctx", "head", None)),
        out_specs=(P("ctx", "head", None), P("ctx", "head", None), P(("ctx", "head"), None)),
        check_vma=False,
    )
```

```python
import jax
import jax.numpy as jnp
from jax import lax
from jax.experimental import pallas as pl
from jax.experimental.pallas import tpu as pltpu
from jax.sharding import PartitionSpec as P

SCALE = 192 ** (-0.5)
LANES = 128
BF = jnp.bfloat16
F32 = jnp.float32
NT = (((1,), (1,)), ((), ()))
NN = (((1,), (0,)), ((), ()))


def dot(a, b, dims):
    return lax.dot_general(a, b, dims, preferred_element_type=F32)


def two_heads(q_ref, h):
    return jnp.concatenate([q_ref[h], q_ref[h + 1]], axis=1)


def own_kernel(q_ref, g_ref, k_ref, qv_ref, kv_ref, gh_ref, s_ref, p_ref, gbuf, wide, sems):
    heads, _, tok = qv_ref.shape
    lat = gh_ref.shape[1]
    parts = lat // LANES
    g_copies = []
    for c in range(parts):
        lanes = slice(c * LANES, (c + 1) * LANES)
        g_copies.append(pltpu.make_async_copy(g_ref.at[:, :, lanes], gbuf.at[:, :, lanes], sems.at[c]))
    q_copies = [pltpu.make_async_copy(q_ref.at[h], qv_ref.at[h], sems.at[parts + h]) for h in range(heads)]
    k_copy = pltpu.make_async_copy(k_ref, kv_ref, sems.at[parts + heads])
    for copy in [k_copy] + g_copies + q_copies:
        copy.start()
    k_copy.wait()
    keys = kv_ref[...].T
    for c in range(parts):
        g_copies[c].wait()
        lanes = slice(c * LANES, (c + 1) * LANES)
        wide[c] = gbuf[:, :, lanes].astype(F32).reshape(tok * heads, LANES)
        for i in range(heads):
            gh_ref[i * tok : (i + 1) * tok, lanes] = wide[c, pl.ds(i, tok, stride=heads), :].astype(BF)
    for h in range(0, heads, 2):
        cols = slice(h * tok, (h + 2) * tok)
        p_ref[:, cols] = dot(keys[:, :lat], gh_ref[cols, :], NT)
    for h in range(0, heads, 2):
        cols = slice(h * tok, (h + 2) * tok)
        for i in (h, h + 1):
            q_copies[i].wait()
        s_ref[:, cols] = dot(keys, two_heads(qv_ref, h), NN)


def visible(ctx_ref, doc_ref, blocks):
    tok = doc_ref.shape[1]
    base = ctx_ref[0] * tok
    row = lax.broadcasted_iota(jnp.int32, (tok, 2 * tok), 0)
    qpos = base + (lax.broadcasted_iota(jnp.int32, (tok, 2 * tok), 1) % tok)
    doc = jnp.concatenate([doc_ref[...], doc_ref[...]], axis=1)
    seen = [(base - back * tok + row >= doc) & (base - back * tok + row <= qpos) for back in blocks]
    return seen


def mid_kernel(ctx_ref, q_ref, gh_ref, s0_ref, p0_ref, k_ref, doc_ref, e_ref, p_ref, top_ref, sum_ref, del_ref):
    heads, _, tok = q_ref.shape
    lat = gh_ref.shape[1]
    keys = k_ref[...].T
    seen = visible(ctx_ref, doc_ref, (2, 0))
    for h in range(0, heads, 2):
        cols = slice(h * tok, (h + 2) * tok)
        far = jnp.where(seen[0], dot(keys, two_heads(q_ref, h), NN) * SCALE, -jnp.inf)
        own = jnp.where(seen[1], s0_ref[:, cols] * SCALE, -jnp.inf)
        s = jnp.concatenate([far, own], axis=0)
        top = jnp.max(s, axis=0, keepdims=True)
        e = jnp.exp(s - top)
        p1 = dot(keys[:, :lat], gh_ref[cols, :], NT)
        dp = jnp.concatenate([p1, p0_ref[:, cols]], axis=0)
        e_ref[:, cols] = e
        p_ref[:, cols] = p1
        top_ref[:, cols] = top
        sum_ref[:, cols] = jnp.sum(e, axis=0, keepdims=True)
        del_ref[:, cols] = jnp.sum(e * dp, axis=0, keepdims=True)


def main_kernel(
    ctx_ref, q_ref, gh_ref, e_ref, p2_ref, top_ref, sum_ref, del_ref, k1_ref, doc_ref, *outs
):
    w_ref, ds_ref, fac_ref, delta_ref, a2_ref, a1_ref = outs
    heads, _, tok = q_ref.shape
    lat = gh_ref.shape[1]
    keys = k1_ref[...].T
    (seen,) = visible(ctx_ref, doc_ref, (1,))
    for h in range(0, heads, 2):
        cols = slice(h * tok, (h + 2) * tok)
        s = jnp.where(seen, dot(keys, two_heads(q_ref, h), NN) * SCALE, -jnp.inf)
        before = top_ref[:, cols]
        top = jnp.maximum(before, jnp.max(s, axis=0, keepdims=True))
        e = jnp.exp(s - top)
        old = jnp.exp(before - top)
        inv = 1.0 / (old * sum_ref[:, cols] + jnp.sum(e, axis=0, keepdims=True))
        dp = dot(keys[:, :lat], gh_ref[cols, :], NT)
        delta = (old * del_ref[:, cols] + jnp.sum(e * dp, axis=0, keepdims=True)) * inv
        prob = e * inv
        w_ref[tok:, cols] = prob.astype(BF)
        ds_ref[tok:, cols] = (SCALE * prob * (dp - delta)).astype(BF)
        fac_ref[:, cols] = old * inv
        delta_ref[:, cols] = delta
        prob = e_ref[:tok, cols] * (old * inv)
        w_ref[:tok, cols] = prob.astype(BF)
        ds_ref[:tok, cols] = (SCALE * prob * (p2_ref[:, cols] - delta)).astype(BF)
    main, rest = partial_grad(w_ref, ds_ref, q_ref, gh_ref)
    put_packed((main[:tok], rest[:tok]), a2_ref, lat)
    put_packed((main[tok:], rest[tok:]), a1_ref, lat)


def partial_grad(w_ref, ds_ref, q_ref, gh_ref):
    heads = q_ref.shape[0]
    lat = gh_ref.shape[1]
    qs = jnp.concatenate([q_ref[h] for h in range(heads)], axis=1)
    score_part = dot(ds_ref[...], qs, NT)
    value_part = dot(w_ref[...], gh_ref[...], NN)
    return score_part[:, :lat] + value_part, score_part[:, lat:]


def put_packed(parts, out_ref, lat):
    main, rest = parts
    tok, width = rest.shape
    fold = LANES // width
    rows = tok // fold
    rest = jnp.concatenate([rest[n * rows : (n + 1) * rows] for n in range(fold)], axis=1)
    count = lat // LANES
    out_ref[:tok, :] = main.astype(BF)
    for n in range(count):
        piece = rest[n * rows // count : (n + 1) * rows // count]
        out_ref[tok:, n * LANES : (n + 1) * LANES] = piece.astype(BF)


def get_packed(ref, tok, width):
    lat = ref.shape[1]
    rest = ref[tok:, :].astype(F32)
    rest = jnp.concatenate([rest[:, n * LANES : (n + 1) * LANES] for n in range(lat // LANES)], axis=0)
    rest = jnp.concatenate([rest[:, n * width : (n + 1) * width] for n in range(LANES // width)], axis=0)
    return ref[:tok, :].astype(F32), rest


def last_kernel(e_ref, p_ref, fac_ref, delta_ref, q_ref, gh_ref, w_ref, ds_ref, o_ref):
    lat = gh_ref.shape[1]
    tok = w_ref.shape[0]
    prob = e_ref[tok:, :] * fac_ref[...]
    w_ref[...] = prob.astype(BF)
    ds_ref[...] = (SCALE * prob * (p_ref[...] - delta_ref[...])).astype(BF)
    main, rest = partial_grad(w_ref, ds_ref, q_ref, gh_ref)
    o_ref[:, :lat] = main
    o_ref[:, lat:] = rest


def add_kernel(own_ref, r2_ref, r1_ref, o_ref):
    tok, width = own_ref.shape
    lat = r2_ref.shape[1]
    main2, rest2 = get_packed(r2_ref, tok, width - lat)
    main1, rest1 = get_packed(r1_ref, tok, width - lat)
    dims = o_ref.shape[:2]
    o_ref[:, :, :lat] = (own_ref[:, :lat] + main2 + main1).reshape(*dims, lat).astype(BF)
    o_ref[:, :, lat:] = (own_ref[:, lat:] + rest2 + rest1).reshape(*dims, width - lat).astype(BF)


def att_kernel(w12_ref, w0_ref, k2_ref, k1_ref, k0_ref, att_ref, wide):
    tok, heads, lat = att_ref.shape
    kt = jnp.concatenate([k2_ref[:lat], k1_ref[:lat], k0_ref[:lat]], axis=1)
    for i in range(heads):
        cols = slice(i * tok, (i + 1) * tok)
        weights = jnp.concatenate([w12_ref[:, cols].T, w0_ref[:, cols].T], axis=1)
        att = dot(weights, kt, NT)
        for c in range(lat // LANES):
            wide[c, pl.ds(i, tok, stride=heads), :] = att[:, c * LANES : (c + 1) * LANES]
    for c in range(lat // LANES):
        att_ref[:, :, c * LANES : (c + 1) * LANES] = wide[c].reshape(tok, heads, LANES).astype(BF)


def dq_kernel(ds12_ref, ds0_ref, k2_ref, k1_ref, k0_ref, dq_ref):
    heads, _, tok = dq_ref.shape
    kt = jnp.concatenate([k2_ref[...], k1_ref[...], k0_ref[...]], axis=1)
    for h in range(0, heads, 2):
        cols = slice(h * tok, (h + 2) * tok)
        ds = jnp.concatenate([ds12_ref[:, cols], ds0_ref[:, cols]], axis=0)
        dq = dot(kt, ds, NN).astype(BF)
        dq_ref[h] = dq[:, :tok]
        dq_ref[h + 1] = dq[:, tok:]


def ctx_pairs(step, ctx_count, head_count, row):
    pairs = []
    for source in range(ctx_count):
        target = source + step
        if 0 <= target < ctx_count:
            flip = source // row != target // row
            for head in range(head_count):
                pairs.append((source * head_count + head, target * head_count + (head ^ 1 if flip else head)))
    return pairs


def in_vmem(*values):
    return tuple(pltpu.with_memory_space_constraint(x, pltpu.VMEM) for x in values)


def call(kernel, out, ins, scratch=()):
    vmem = pl.BlockSpec(memory_space=pltpu.VMEM)
    specs = {"smem": pl.BlockSpec(memory_space=pltpu.SMEM), "hbm": pl.BlockSpec(memory_space=pltpu.HBM)}
    return pl.pallas_call(
        kernel,
        out_shape=out,
        in_specs=[specs.get(where, vmem) for where, _ in ins],
        out_specs=jax.tree.map(lambda _: vmem, out),
        scratch_shapes=scratch,
        compiler_params=pltpu.CompilerParams(vmem_limit_bytes=16 << 20),
    )(*[value for _, value in ins])


def v(*values):
    return [("vmem", value) for value in values]


def step(query_heads, key_latent, doc_start, out_grad):
    tok, heads, width = query_heads.shape
    lat = out_grad.shape[2]
    ctx_count = lax.axis_size("ctx")
    head_count = lax.axis_size("head")
    both = ("ctx", "head")
    rows = tok * heads
    packed = (tok * width // lat, lat)
    mem = pltpu.VMEM
    shape = jax.ShapeDtypeStruct

    def shift(value, steps):
        return lax.ppermute(value, both, ctx_pairs(steps, ctx_count, head_count, 16))

    ctx = ("smem", lax.axis_index("ctx").astype(jnp.int32).reshape(1))
    doc = doc_start.reshape(1, tok)
    kt = key_latent.T
    k2 = shift(kt, 2)
    k1 = shift(kt, 1)
    k2, k1 = in_vmem(k2, k1)
    qt = jnp.transpose(query_heads, (1, 2, 0))
    qt, og, kt = (pltpu.with_memory_space_constraint(x, pltpu.HBM) for x in (qt, out_grad, kt))
    wide_buf = mem((lat // LANES, rows, LANES), F32)
    qv, k0, gh, s0, p0 = call(
        own_kernel,
        (
            mem((heads, width, tok), BF),
            mem((width, tok), BF),
            mem((rows, lat), BF),
            mem((tok, rows), F32),
            mem((tok, rows), F32),
        ),
        [("hbm", qt), ("hbm", og), ("hbm", kt)],
        (mem((tok, heads, lat), BF), wide_buf, pltpu.SemaphoreType.DMA((lat // LANES + heads + 1,))),
    )
    row = mem((1, rows), F32)
    e, p2, top, total, part = call(
        mid_kernel,
        (mem((2 * tok, rows), F32), mem((tok, rows), F32), row, row, row),
        [ctx] + v(qv, gh, s0, p0, k2, doc),
    )
    tile = mem((tok, rows), BF)
    pair = mem((2 * tok, rows), BF)
    w12, ds12, fac, delta, a2, a1 = call(
        main_kernel,
        (pair, pair, row, row, mem(packed, BF), mem(packed, BF)),
        [ctx] + v(qv, gh, e, p2, top, total, part, k1, doc),
    )
    r2 = shift(a2, -2)
    r1 = shift(a1, -1)
    w0, ds0, own = call(last_kernel, (tile, tile, mem((tok, width), F32)), v(e, p0, fac, delta, qv, gh))
    att = call(att_kernel, shape((tok, heads, lat), BF), v(w12, w0, k2, k1, k0), (wide_buf,))
    dq = call(dq_kernel, shape((heads, width, tok), BF), v(ds12, ds0, k2, k1, k0))
    r2, r1 = in_vmem(r2, r1)
    fours = head_count // 2
    owned = call(add_kernel, mem((fours, tok // fours, width), BF), v(own, r2, r1))
    groups = [[2 * y + z for y in range(fours)] for z in range(2)]
    pieces = lax.all_to_all(owned, "head", 0, 0, axis_index_groups=groups, tiled=True)
    halves = jnp.sum(pieces.astype(F32), axis=0).reshape(2, tok // head_count, width)
    z = lax.axis_index("head") % 2
    mine = jnp.where(z == 0, halves[0], halves[1])
    other = jnp.where(z == 0, halves[1], halves[0]).astype(BF)
    pairs = [[2 * y, 2 * y + 1] for y in range(fours)]
    got = lax.all_gather(other, "head", axis_index_groups=pairs)
    d_key = mine + jnp.where(z == 0, got[1], got[0]).astype(F32)
    return (att, jnp.transpose(dq, (2, 0, 1)), d_key)


def solution(mesh):
    return jax.shard_map(
        step,
        mesh=mesh,
        in_specs=(P("ctx", "head", None), P("ctx", None), P("ctx"), P("ctx", "head", None)),
        out_specs=(P("ctx", "head", None), P("ctx", "head", None), P(("ctx", "head"), None)),
        check_vma=False,
    )
```
